32 devices in a mesh: fact: 8 (over z, x), dim: 4 (over y, core).
Axes of the slice: x: 2, y: 2, z: 4, core: 2. Of those that a mesh axis runs over, the one named last changes fastest.
Arguments:
- fact_keys: int32 [1048576], P(('fact', 'dim')), may hold values from 0 to 65535, as said below
- revenue: bfloat16 [1048576], P(('fact', 'dim')), may hold values from 0.099609375 to 1
- filter_bits: int32 [256, 256], replicated, may hold values from 0 to 1
- categories: int32 [65536], P(('fact', 'dim')), may hold values from 0 to 511
- attributes: bfloat16 [65536, 128], P(('fact', 'dim')), may hold values from -0.125 to 0.125
Outputs:
- category_totals: float32 [512, 128], P(('fact', 'dim'))
The draws below stay inside these ranges and needn't reach their ends.
Inputs may be any that keep to these rules, and one draw needn't show every extreme that they name: `fact_keys`: keys of owner o are o * 2048 to (o + 1) * 2048 - 1. Among the 32768 rows of one device at most 2048 have keys of any one owner; in every draw one owner gets exactly 2048 matching rows from every device, and every device has exactly 2048 matching rows for some owner.
All inputs are finite; a program needn't handle non-finite values.
Results may differ from the reference program's by a relative error of at most 0.0003.
Values may be sent and summed in bfloat16 or wider, within the bound.
A program may use at most 64 MiB of HBM per device.

```python
import math
import jax
import jax.numpy as jnp

KEYS = 65536
KEY_LO = 256
KEY_HI = 256
ATTR = 128
CATS = 512
FACT_DEV = 32768
FACT_ROWS = 1048576
KEYS_OWN = 2048
CAP = 2048
N_FACT = 8
N_DIM = 4


def layout(key):
    devices = N_FACT * N_DIM
    first, second, third, fourth = jax.random.split(jax.random.fold_in(key, 7), 4)
    common = jax.random.randint(first, (), 0, devices)
    picked_all = jax.random.randint(second, (devices,), 0, devices)

    def one_device(device_key, picked):
        key_a, key_b, key_c = jax.random.split(device_key, 3)
        slot_owner = jnp.arange(devices * CAP, dtype=jnp.int32) // CAP
        score = jax.random.permutation(key_a, devices * CAP).astype(jnp.int32)
        forced = (slot_owner == common) | (slot_owner == picked)
        score = jnp.where(forced, score - devices * CAP, score)
        order = jnp.argsort(score, stable=True)[:FACT_DEV]
        owners = jax.random.permutation(key_b, slot_owner[order])
        local = jax.random.randint(key_c, (FACT_DEV,), 0, KEYS_OWN)
        is_forced = (owners == common) | (owners == picked)
        return (owners * KEYS_OWN + local, is_forced)
    keys, forced = jax.vmap(one_device)(jax.random.split(third, devices), picked_all)
    levels = jax.random.randint(fourth, (KEYS,), 0, 4)
    bits = (levels > 0).astype(jnp.int32)
    marks = jnp.where(forced, keys, KEYS).reshape(-1)
    bits = bits.at[marks].set(1, mode='drop')
    return (keys.reshape(-1).astype(jnp.int32), bits.reshape(KEY_HI, KEY_LO).astype(jnp.int32))


def draw_fact_keys(key, part):
    return layout(key)[0]


def draw_filter_bits(key, part):
    return layout(key)[1]


def plant(drawn, key, smallest, top_value):
    dims = drawn.shape
    place = [jax.random.randint(jax.random.fold_in(key, axis), (), 0, dims[axis]) for axis in range(len(dims))]
    drawn = drawn.at[tuple(place)].set(smallest)
    longest = dims.index(max(dims))
    place[longest] = (place[longest] + 1) % dims[longest]
    return drawn.at[tuple(place)].set(top_value)


def shard_levels(stream_key, extent, cuts, least, largest):
    def one(dim, blocks):
        draws = jax.random.uniform(jax.random.fold_in(jax.random.fold_in(stream_key, 6), dim), (blocks,), jnp.float32, least / len(cuts), largest / len(cuts))
        return jnp.repeat(jnp.exp(draws), extent[dim] // blocks).reshape((-1,) + (1,) * (len(extent) - dim - 1))

    gain = one(*cuts[0])
    for cut in cuts[1:]:
        gain = gain * one(*cut)
    return gain


def normal_values(key, extent, scale, reach, cuts=(), kind=jnp.bfloat16):
    entries = scale * jax.random.normal(key, extent, jnp.float32)
    if cuts:
        entries = entries * shard_levels(key, extent, cuts, -0.22, 0.18)
    return jnp.clip(entries, -reach, reach).astype(kind)


def setup_inputs(seed: int = 0) -> dict:
    key_of = jax.random.split(jax.random.key(seed), 6)
    fact_keys = draw_fact_keys(jax.random.fold_in(key_of[5], 71), 0)
    revenue = jnp.clip(jnp.exp(math.log(1.0) - 2.306499 * jax.random.uniform(key_of[1], (FACT_ROWS,), jnp.float32) ** shard_levels(key_of[1], (FACT_ROWS,), ((0, 32),), -0.2, 0.2)), 0.099609375, 1.0).astype(jnp.bfloat16)
    filter_bits = draw_filter_bits(jax.random.fold_in(key_of[5], 71), 0)
    categories = plant(jax.random.randint(key_of[3], (KEYS,), 0, CATS), jax.random.fold_in(key_of[3], 1), 0, CATS - 1).astype(jnp.int32)
    attributes = normal_values(key_of[4], (KEYS, ATTR), (FACT_DEV * N_FACT * N_DIM // CATS) ** -0.5, 0.125, ((0, 32),))
    return dict(fact_keys=fact_keys, revenue=revenue, filter_bits=filter_bits, categories=categories, attributes=attributes)


def reference(fact_keys, revenue, filter_bits, categories, attributes):
    match = filter_bits.reshape(-1)[fact_keys]
    weight = jnp.where(match == 1, revenue.astype(jnp.float32), jnp.float32(0.0))
    key_revenue = jax.ops.segment_sum(weight, fact_keys, num_segments=KEYS)
    weighted = key_revenue[:, None] * attributes.astype(jnp.float32)
    return jax.ops.segment_sum(weighted, categories, num_segments=CATS)
```

```python
import functools

import jax
import jax.numpy as jnp
from jax import lax
from jax.experimental import pallas as pl
from jax.experimental.pallas import tpu as pltpu
from jax.sharding import PartitionSpec as P

CATS = 512
LANES = 128
MESH = pl.DeviceIdType.MESH


def rows_of(row, count):
    packed = jnp.broadcast_to(row, (16, LANES)).astype(jnp.bfloat16)
    return jnp.concatenate([packed] * (count // 16), axis=0)


def ids_of(count):
    return lax.broadcasted_iota(jnp.int32, (count, LANES), 0).astype(jnp.float32).astype(jnp.bfloat16)


def kernel(
    n_fact,
    n_dim,
    keys_ref,
    rev_ref,
    filt_ref,
    cat_ref,
    attr_ref,
    out_ref,
    high_ref,
    low_ref,
    value_ref,
    acc_ref,
    send1,
    recv1,
    weight_ref,
    send2,
    recv2,
    send_sem1,
    recv_sem1,
    send_sem2,
    recv_sem2,
):
    n = n_fact * n_dim
    me = lax.axis_index("fact") * n_dim + lax.axis_index("dim")
    key_hi, key_lo = acc_ref.shape
    own_rows = key_hi // n
    cat_rows = CATS // n

    def device(peer):
        return (peer // n_dim, lax.rem(peer, n_dim))

    def peer_at(step):
        return lax.rem(me + step, n)

    barrier = pltpu.get_barrier_semaphore()

    def greet(step, carry):
        pl.semaphore_signal(barrier, inc=1, device_id=device(peer_at(step)), device_id_type=MESH)
        return carry

    lax.fori_loop(1, n, greet, 0)

    keys = keys_ref[...]
    high_ref[...] = (keys // key_lo).astype(jnp.float32)
    low_ref[...] = lax.rem(keys, key_lo).astype(jnp.float32)
    value_ref[...] = rev_ref[...].astype(jnp.float32)
    acc_ref[...] = jnp.zeros_like(acc_ref)

    lines = keys_ref.shape[0]
    step_lines = 8
    one = jnp.ones((), jnp.bfloat16)
    zero = jnp.zeros((), jnp.bfloat16)

    def add_block(block, carry):
        high_ids = ids_of(key_hi)
        low_ids = ids_of(key_lo)
        hots, weighted = [], []
        for j in range(step_lines):
            line = pl.ds(block * step_lines + j, 1)
            high = rows_of(high_ref[line, :], key_hi)
            low = rows_of(low_ref[line, :], key_lo)
            value = rows_of(value_ref[line, :], key_lo)
            hots.append(jnp.where(high == high_ids, one, zero))
            weighted.append(jnp.where(low == low_ids, value, zero))
        acc_ref[...] += lax.dot_general(
            jnp.concatenate(hots, axis=1),
            jnp.concatenate(weighted, axis=1),
            (((1,), (1,)), ((), ())),
            preferred_element_type=jnp.float32,
        )
        return carry

    lax.fori_loop(0, lines // step_lines, add_block, 0)

    for o in range(n):
        send1[o] = acc_ref[o * own_rows : (o + 1) * own_rows, :]

    pl.semaphore_wait(barrier, n - 1)

    def exchange(send, recv, send_sem, recv_sem):
        def copy_to(peer):
            return pltpu.make_async_remote_copy(
                src_ref=send.at[peer],
                dst_ref=recv.at[me],
                send_sem=send_sem.at[peer],
                recv_sem=recv_sem.at[me],
                device_id=device(peer),
                device_id_type=MESH,
            )

        def start(step, carry):
            copy_to(peer_at(step)).start()
            return carry

        lax.fori_loop(1, n, start, 0)

        def receive(step, total):
            peer = lax.rem(me + n - step, n)
            pltpu.make_async_remote_copy(
                src_ref=send.at[peer],
                dst_ref=recv.at[peer],
                send_sem=send_sem.at[peer],
                recv_sem=recv_sem.at[peer],
                device_id=device(peer),
                device_id_type=MESH,
            ).wait_recv()
            return total + recv[peer]

        total = lax.fori_loop(1, n, receive, send[me])

        def finish():
            def wait(step, carry):
                copy_to(peer_at(step)).wait_send()
                return carry

            lax.fori_loop(1, n, wait, 0)

        return total, finish

    sums, finish1 = exchange(send1, recv1, send_sem1, recv_sem1)
    sums = jnp.where(filt_ref[me] == 1, sums, 0.0)

    half = CATS // 2
    ids = ids_of(half)
    per_row = key_lo // LANES
    for j in range(own_rows * per_row):
        r, c = j // per_row, j % per_row
        own = sums[r : r + 1, c * LANES : (c + 1) * LANES]
        cat = cat_ref[j : j + 1, :]
        upper = cat >= half
        match = rows_of(jnp.where(upper, cat - half, cat).astype(jnp.float32), half) == ids
        first = own.astype(jnp.bfloat16).astype(jnp.float32)
        for t, term in enumerate((first, own - first)):
            for h in range(2):
                part = jnp.where(upper == (h == 1), term, 0.0)
                base = t * CATS + h * half
                weight_ref[base : base + half, j * LANES : (j + 1) * LANES] = jnp.where(
                    match, rows_of(part, half), zero
                )
    attrs = attr_ref[...]
    totals = jnp.dot(
        weight_ref[:CATS, :], attrs, preferred_element_type=jnp.float32
    ) + jnp.dot(weight_ref[CATS:, :], attrs, preferred_element_type=jnp.float32)
    for o in range(n):
        send2[o] = totals[o * cat_rows : (o + 1) * cat_rows, :]
    result, finish2 = exchange(send2, recv2, send_sem2, recv_sem2)
    out_ref[...] = result
    finish1()
    finish2()


def solution(mesh):
    n_fact, n_dim = mesh.shape["fact"], mesh.shape["dim"]
    n = n_fact * n_dim

    def per_device(fact_keys, revenue, filter_bits, categories, attributes):
        rows = fact_keys.shape[0]
        key_hi, key_lo = filter_bits.shape
        own, width = attributes.shape
        lines = rows // LANES
        sums_shape = (n, key_hi // n, key_lo)
        part_shape = (n, CATS // n, width)
        vmem = pl.BlockSpec(memory_space=pltpu.VMEM)
        return pl.pallas_call(
            functools.partial(kernel, n_fact, n_dim),
            out_shape=jax.ShapeDtypeStruct((CATS // n, width), jnp.float32),
            in_specs=[vmem] * 5,
            out_specs=vmem,
            scratch_shapes=[
                pltpu.VMEM((lines, LANES), jnp.float32),
                pltpu.VMEM((lines, LANES), jnp.float32),
                pltpu.VMEM((lines, LANES), jnp.float32),
                pltpu.VMEM((key_hi, key_lo), jnp.float32),
                pltpu.VMEM(sums_shape, jnp.float32),
                pltpu.VMEM(sums_shape, jnp.float32),
                pltpu.VMEM((2 * CATS, own), jnp.bfloat16),
                pltpu.VMEM(part_shape, jnp.float32),
                pltpu.VMEM(part_shape, jnp.float32),
                pltpu.SemaphoreType.DMA((n,)),
                pltpu.SemaphoreType.DMA((n,)),
                pltpu.SemaphoreType.DMA((n,)),
                pltpu.SemaphoreType.DMA((n,)),
            ],
            compiler_params=pltpu.CompilerParams(collective_id=0, has_side_effects=True),
        )(
            fact_keys.reshape(lines, LANES),
            revenue.reshape(lines, LANES),
            filter_bits.reshape(n, key_hi // n, key_lo),
            categories.reshape(own // LANES, LANES),
            attributes,
        )

    split = P(("fact", "dim"))
    return jax.shard_map(
        per_device,
        mesh=mesh,
        in_specs=(split, split, P(), split, P(("fact", "dim"), None)),
        out_specs=P(("fact", "dim"), None),
        check_vma=False,
    )
```

```python
import functools

import jax
import jax.numpy as jnp
from jax import lax
from jax.experimental import pallas as pl
from jax.experimental.pallas import tpu as pltpu
from jax.sharding import PartitionSpec as P

CATS = 512
LANES = 128
MESH = pl.DeviceIdType.MESH


def rows_of(row, count):
    packed = jnp.broadcast_to(row, (16, LANES)).astype(jnp.bfloat16)
    return jnp.concatenate([packed] * (count // 16), axis=0)


def ids_of(count):
    return lax.broadcasted_iota(jnp.int32, (count, LANES), 0).astype(jnp.float32).astype(jnp.bfloat16)


def kernel(
    n_fact,
    n_dim,
    keys_ref,
    rev_ref,
    filt_hbm,
    cat_hbm,
    attr_hbm,
    out_ref,
    high_ref,
    low_ref,
    value_ref,
    acc_ref,
    filt_ref,
    cat_ref,
    attr_ref,
    weight_ref,
    local1,
    pair1,
    send1,
    recv1,
    local2,
    pair2,
    send2,
    recv2,
    load_sem,
    pair_sem,
    send_sem1,
    recv_sem1,
    send_sem2,
    recv_sem2,
):
    n = n_fact * n_dim
    chips = n // 2
    me = lax.axis_index("fact") * n_dim + lax.axis_index("dim")
    core, chip = lax.rem(me, 2), me // 2
    partner = me + 1 - 2 * core
    key_hi, key_lo = acc_ref.shape
    own_rows = key_hi // n
    cat_rows = CATS // n

    def device(peer):
        return (peer // n_dim, lax.rem(peer, n_dim))

    bits = [1 << b for b in range(chips.bit_length() - 1)]
    flips = chips == 1 << len(bits)

    def chip_at(step):
        if not flips:
            return lax.rem(chip + step, chips)
        peer = 0
        for bit in bits:
            digit = lax.rem(chip // bit, 2)
            peer += (1 - digit if step & bit else digit) * bit
        return peer

    def source_at(step):
        return chip_at(step) if flips else lax.rem(chip + chips - step, chips)

    targets = [chip_at(step) for step in range(1, chips)][::-1]
    sources = [source_at(step) for step in range(1, chips)]

    loads = [
        pltpu.make_async_copy(attr_hbm, attr_ref, load_sem.at[0]),
        pltpu.make_async_copy(filt_hbm.at[me], filt_ref, load_sem.at[1]),
        pltpu.make_async_copy(cat_hbm, cat_ref, load_sem.at[2]),
    ]
    for load in loads:
        load.start()

    barrier = pltpu.get_barrier_semaphore()
    for peer in [partner] + [t * 2 + core for t in targets]:
        pl.semaphore_signal(barrier, inc=1, device_id=device(peer), device_id_type=MESH)

    keys = keys_ref[...]
    high_ref[...] = (keys // key_lo).astype(jnp.float32)
    low_ref[...] = lax.rem(keys, key_lo).astype(jnp.float32)
    value_ref[...] = rev_ref[...].astype(jnp.float32)
    acc_ref[...] = jnp.zeros_like(acc_ref)

    lines = keys_ref.shape[0]
    step_lines = 8
    one = jnp.ones((), jnp.bfloat16)
    zero = jnp.zeros((), jnp.bfloat16)

    def add_block(block, carry):
        high_ids = ids_of(key_hi)
        low_ids = ids_of(key_lo)
        hots, weighted = [], []
        for j in range(step_lines):
            line = pl.ds(block * step_lines + j, 1)
            high = rows_of(high_ref[line, :], key_hi)
            low = rows_of(low_ref[line, :], key_lo)
            value = rows_of(value_ref[line, :], key_lo)
            hots.append(jnp.where(high == high_ids, one, zero))
            weighted.append(jnp.where(low == low_ids, value, zero))
        acc_ref[...] += lax.dot_general(
            jnp.concatenate(hots, axis=1),
            jnp.concatenate(weighted, axis=1),
            (((1,), (1,)), ((), ())),
            preferred_element_type=jnp.float32,
        )
        return carry

    lax.fori_loop(0, lines // step_lines, add_block, 0)

    for o in range(n):
        local1[o % 2, o // 2] = acc_ref[o * own_rows : (o + 1) * own_rows, :]

    pl.semaphore_wait(barrier, chips)

    def exchange(local, pair, send, recv, sems, send_sem, recv_sem):
        swap = pltpu.make_async_remote_copy(
            src_ref=local.at[1 - core],
            dst_ref=pair,
            send_sem=pair_sem.at[sems],
            recv_sem=pair_sem.at[sems + 1],
            device_id=device(partner),
            device_id_type=MESH,
        )
        swap.start()
        swap.wait_recv()
        send[...] = local[core] + pair[...]
        copies = [
            pltpu.make_async_remote_copy(
                src_ref=send.at[peer],
                dst_ref=recv.at[chip],
                send_sem=send_sem.at[peer],
                recv_sem=recv_sem.at[chip],
                device_id=device(peer * 2 + core),
                device_id_type=MESH,
            )
            for peer in targets
        ]
        for copy in copies:
            copy.start()

        def receive():
            total = send[chip]
            for peer in sources:
                pltpu.make_async_remote_copy(
                    src_ref=send.at[peer],
                    dst_ref=recv.at[peer],
                    send_sem=send_sem.at[peer],
                    recv_sem=recv_sem.at[peer],
                    device_id=device(peer * 2 + core),
                    device_id_type=MESH,
                ).wait_recv()
                total += recv[peer]
            return total

        def finish():
            swap.wait_send()
            for copy in copies:
                copy.wait_send()

        return receive, finish

    receive1, finish1 = exchange(local1, pair1, send1, recv1, 0, send_sem1, recv_sem1)
    for load in loads:
        load.wait()
    sums = jnp.where(filt_ref[...] == 1, receive1(), 0.0)

    half = CATS // 2
    ids = ids_of(half)
    per_row = key_lo // LANES
    for j in range(own_rows * per_row):
        r, c = j // per_row, j % per_row
        own = sums[r : r + 1, c * LANES : (c + 1) * LANES]
        cat = cat_ref[j : j + 1, :]
        upper = cat >= half
        match = rows_of(jnp.where(upper, cat - half, cat).astype(jnp.float32), half) == ids
        first = own.astype(jnp.bfloat16).astype(jnp.float32)
        for t, term in enumerate((first, own - first)):
            for h in range(2):
                part = jnp.where(upper == (h == 1), term, 0.0)
                base = t * CATS + h * half
                weight_ref[base : base + half, j * LANES : (j + 1) * LANES] = jnp.where(
                    match, rows_of(part, half), zero
                )
    attrs = attr_ref[...]
    totals = jnp.dot(
        weight_ref[:CATS, :], attrs, preferred_element_type=jnp.float32
    ) + jnp.dot(weight_ref[CATS:, :], attrs, preferred_element_type=jnp.float32)
    for o in range(n):
        local2[o % 2, o // 2] = totals[o * cat_rows : (o + 1) * cat_rows, :]
    receive2, finish2 = exchange(local2, pair2, send2, recv2, 2, send_sem2, recv_sem2)
    finish1()
    out_ref[...] = receive2()
    finish2()


def solution(mesh):
    n_fact, n_dim = mesh.shape["fact"], mesh.shape["dim"]
    n = n_fact * n_dim

    def per_device(fact_keys, revenue, filter_bits, categories, attributes):
        rows = fact_keys.shape[0]
        key_hi, key_lo = filter_bits.shape
        own, width = attributes.shape
        lines = rows // LANES
        chips = n // 2
        sums_shape = (chips, key_hi // n, key_lo)
        part_shape = (chips, CATS // n, width)
        vmem = pl.BlockSpec(memory_space=pltpu.VMEM)
        hbm = pl.BlockSpec(memory_space=pl.ANY)
        exchanged = []
        for shape in (sums_shape, part_shape):
            exchanged.append(pltpu.VMEM((2,) + shape, jnp.float32))
            exchanged += [pltpu.VMEM(shape, jnp.float32)] * 3
        return pl.pallas_call(
            functools.partial(kernel, n_fact, n_dim),
            out_shape=jax.ShapeDtypeStruct((CATS // n, width), jnp.float32),
            in_specs=[vmem, vmem, hbm, hbm, hbm],
            out_specs=vmem,
            scratch_shapes=[
                pltpu.VMEM((lines, LANES), jnp.float32),
                pltpu.VMEM((lines, LANES), jnp.float32),
                pltpu.VMEM((lines, LANES), jnp.float32),
                pltpu.VMEM((key_hi, key_lo), jnp.float32),
                pltpu.VMEM((key_hi // n, key_lo), jnp.int32),
                pltpu.VMEM((own // LANES, LANES), jnp.int32),
                pltpu.VMEM((own, width), jnp.bfloat16),
                pltpu.VMEM((2 * CATS, own), jnp.bfloat16),
            ]
            + exchanged
            + [pltpu.SemaphoreType.DMA((3,)), pltpu.SemaphoreType.DMA((4,))]
            + [pltpu.SemaphoreType.DMA((chips,))] * 4,
            compiler_params=pltpu.CompilerParams(collective_id=0, has_side_effects=True),
        )(
            fact_keys.reshape(lines, LANES),
            revenue.reshape(lines, LANES),
            filter_bits.reshape(n, key_hi // n, key_lo),
            categories.reshape(own // LANES, LANES),
            attributes,
        )

    split = P(("fact", "dim"))
    return jax.shard_map(
        per_device,
        mesh=mesh,
        in_specs=(split, split, P(), split, P(("fact", "dim"), None)),
        out_specs=P(("fact", "dim"), None),
        check_vma=False,
    )
```

```python
import functools
import math

import jax
import jax.numpy as jnp
from jax import lax
from jax.experimental import pallas as pl
from jax.experimental.pallas import tpu as pltpu
from jax.sharding import PartitionSpec as P

CATS = 512
LANES = 128
MESH = pl.DeviceIdType.MESH


def rows_of(row, count):
    packed = jnp.broadcast_to(row, (16, LANES)).astype(jnp.bfloat16)
    return jnp.concatenate([packed] * (count // 16), axis=0)


def ids_of(count):
    return lax.broadcasted_iota(jnp.int32, (count, LANES), 0).astype(jnp.float32).astype(jnp.bfloat16)


def kernel(
    n_fact,
    n_dim,
    keys_hbm,
    rev_hbm,
    filt_hbm,
    cat_hbm,
    attr_hbm,
    out_ref,
    keys_ref,
    rev_ref,
    high_ref,
    low_ref,
    value_ref,
    acc_ref,
    filt_ref,
    cat_ref,
    attr_ref,
    hot_ref,
    weight_ref,
    local1,
    pair1,
    send1,
    recv1,
    local2,
    pair2,
    send2,
    recv2,
    load_sem,
    pair_sem,
    send_sem1,
    recv_sem1,
    send_sem2,
    recv_sem2,
):
    n = n_fact * n_dim
    chips = n // 2
    me = lax.axis_index("fact") * n_dim + lax.axis_index("dim")
    core, chip = lax.rem(me, 2), me // 2
    partner = me + 1 - 2 * core
    key_hi, key_lo = acc_ref.shape
    own_rows = key_hi // n
    cat_rows = CATS // n

    def device(peer):
        return (peer // n_dim, lax.rem(peer, n_dim))

    bits = [1 << b for b in range(chips.bit_length() - 1)]
    flips = chips == 1 << len(bits)

    def chip_at(step):
        if not flips:
            return lax.rem(chip + step, chips)
        peer = 0
        for bit in bits:
            digit = lax.rem(chip // bit, 2)
            peer += (1 - digit if step & bit else digit) * bit
        return peer

    def source_at(step):
        return chip_at(step) if flips else lax.rem(chip + chips - step, chips)

    targets = [chip_at(step) for step in range(1, chips)][::-1]
    sources = [source_at(step) for step in range(1, chips)]

    first_loads = [
        pltpu.make_async_copy(keys_hbm, keys_ref, load_sem.at[3]),
        pltpu.make_async_copy(rev_hbm, rev_ref, load_sem.at[4]),
    ]
    for load in first_loads:
        load.start()
    loads = [
        pltpu.make_async_copy(attr_hbm, attr_ref, load_sem.at[0]),
        pltpu.make_async_copy(filt_hbm.at[me], filt_ref, load_sem.at[1]),
        pltpu.make_async_copy(cat_hbm, cat_ref, load_sem.at[2]),
    ]
    barrier = pltpu.get_barrier_semaphore()
    for peer in [partner] + [t * 2 + core for t in targets]:
        pl.semaphore_signal(barrier, inc=1, device_id=device(peer), device_id_type=MESH)

    for load in loads:
        load.start()
    for load in first_loads:
        load.wait()
    keys = keys_ref[...]
    high_ref[...] = (keys // key_lo).astype(jnp.float32)
    low_ref[...] = lax.rem(keys, key_lo).astype(jnp.float32)
    value_ref[...] = rev_ref[...].astype(jnp.float32)
    acc_ref[...] = jnp.zeros_like(acc_ref)

    lines = keys_ref.shape[0]
    step_lines = math.gcd(lines, 64)
    one = jnp.ones((), jnp.bfloat16)
    zero = jnp.zeros((), jnp.bfloat16)

    def add_block(block, carry):
        high_ids = ids_of(key_hi)
        low_ids = ids_of(key_lo)
        hots, weighted = [], []
        for j in range(step_lines):
            line = pl.ds(block * step_lines + j, 1)
            high = rows_of(high_ref[line, :], key_hi)
            low = rows_of(low_ref[line, :], key_lo)
            value = rows_of(value_ref[line, :], key_lo)
            hots.append(jnp.where(high == high_ids, one, zero))
            weighted.append(jnp.where(low == low_ids, value, zero))
        acc_ref[...] += lax.dot_general(
            jnp.concatenate(hots, axis=1),
            jnp.concatenate(weighted, axis=1),
            (((1,), (1,)), ((), ())),
            preferred_element_type=jnp.float32,
        )
        return carry

    lax.fori_loop(0, lines // step_lines, add_block, 0)

    for o in range(n):
        local1[o % 2, o // 2] = acc_ref[o * own_rows : (o + 1) * own_rows, :]

    pl.semaphore_wait(barrier, chips)

    def exchange(local, pair, send, recv, sems, send_sem, recv_sem):
        swap = pltpu.make_async_remote_copy(
            src_ref=local.at[1 - core],
            dst_ref=pair,
            send_sem=pair_sem.at[sems],
            recv_sem=pair_sem.at[sems + 1],
            device_id=device(partner),
            device_id_type=MESH,
        )
        swap.start()
        swap.wait_recv()
        send[...] = local[core] + pair[...]
        copies = [
            pltpu.make_async_remote_copy(
                src_ref=send.at[peer],
                dst_ref=recv.at[chip],
                send_sem=send_sem.at[peer],
                recv_sem=recv_sem.at[chip],
                device_id=device(peer * 2 + core),
                device_id_type=MESH,
            )
            for peer in targets
        ]
        for copy in copies:
            copy.start()

        def receive():
            total = send[chip]
            for peer in sources:
                pltpu.make_async_remote_copy(
                    src_ref=send.at[peer],
                    dst_ref=recv.at[peer],
                    send_sem=send_sem.at[peer],
                    recv_sem=recv_sem.at[peer],
                    device_id=device(peer * 2 + core),
                    device_id_type=MESH,
                ).wait_recv()
                total += recv[peer]
            return total

        def finish():
            swap.wait_send()
            for copy in copies:
                copy.wait_send()

        return receive, finish

    receive1, finish1 = exchange(local1, pair1, send1, recv1, 0, send_sem1, recv_sem1)
    for load in loads:
        load.wait()

    half = CATS // 2
    ids = ids_of(half)
    per_row = key_lo // LANES
    chunks = own_rows * per_row
    for j in range(chunks):
        cat = cat_ref[j : j + 1, :]
        for h, local in enumerate((jnp.where(cat < half, cat, -1), cat - half)):
            hot_ref[h * half : (h + 1) * half, j * LANES : (j + 1) * LANES] = jnp.where(
                rows_of(local.astype(jnp.float32), half) == ids, one, zero
            )

    sums = jnp.where(filt_ref[...] == 1, receive1(), 0.0)
    stacked = [sums[:, c * LANES : (c + 1) * LANES] for c in range(per_row)]
    stacked.append(jnp.zeros((LANES - chunks, LANES), jnp.float32))
    columns = jnp.concatenate(stacked, axis=0).T
    width = attr_ref.shape[1]
    for j in range(chunks):
        i = j % per_row * own_rows + j // per_row
        keys_at = slice(j * LANES, (j + 1) * LANES)
        product = columns[:, i : i + 1] * attr_ref[keys_at, :].astype(jnp.float32)
        first = product.astype(jnp.bfloat16)
        weight_ref[keys_at, :width] = first
        weight_ref[keys_at, width:] = (product - first.astype(jnp.float32)).astype(jnp.bfloat16)
    both = jnp.dot(hot_ref[...], weight_ref[...], preferred_element_type=jnp.float32)
    totals = both[:, :width] + both[:, width:]
    for o in range(n):
        local2[o % 2, o // 2] = totals[o * cat_rows : (o + 1) * cat_rows, :]
    receive2, finish2 = exchange(local2, pair2, send2, recv2, 2, send_sem2, recv_sem2)
    finish1()
    out_ref[...] = receive2()
    finish2()


def solution(mesh):
    n_fact, n_dim = mesh.shape["fact"], mesh.shape["dim"]
    n = n_fact * n_dim

    def per_device(fact_keys, revenue, filter_bits, categories, attributes):
        rows = fact_keys.shape[0]
        key_hi, key_lo = filter_bits.shape
        own, width = attributes.shape
        lines = rows // LANES
        chips = n // 2
        sums_shape = (chips, key_hi // n, key_lo)
        part_shape = (chips, CATS // n, width)
        vmem = pl.BlockSpec(memory_space=pltpu.VMEM)
        hbm = pl.BlockSpec(memory_space=pl.ANY)
        exchanged = []
        for shape in (sums_shape, part_shape):
            exchanged.append(pltpu.VMEM((2,) + shape, jnp.float32))
            exchanged += [pltpu.VMEM(shape, jnp.float32)] * 3
        return pl.pallas_call(
            functools.partial(kernel, n_fact, n_dim),
            out_shape=jax.ShapeDtypeStruct((CATS // n, width), jnp.float32),
            in_specs=[hbm] * 5,
            out_specs=vmem,
            scratch_shapes=[
                pltpu.VMEM((lines, LANES), jnp.int32),
                pltpu.VMEM((lines, LANES), jnp.bfloat16),
                pltpu.VMEM((lines, LANES), jnp.float32),
                pltpu.VMEM((lines, LANES), jnp.float32),
                pltpu.VMEM((lines, LANES), jnp.float32),
                pltpu.VMEM((key_hi, key_lo), jnp.float32),
                pltpu.VMEM((key_hi // n, key_lo), jnp.int32),
                pltpu.VMEM((own // LANES, LANES), jnp.int32),
                pltpu.VMEM((own, width), jnp.bfloat16),
                pltpu.VMEM((CATS, own), jnp.bfloat16),
                pltpu.VMEM((own, 2 * width), jnp.bfloat16),
            ]
            + exchanged
            + [pltpu.SemaphoreType.DMA((5,)), pltpu.SemaphoreType.DMA((4,))]
            + [pltpu.SemaphoreType.DMA((chips,))] * 4,
            compiler_params=pltpu.CompilerParams(collective_id=0, has_side_effects=True),
        )(
            fact_keys.reshape(lines, LANES),
            revenue.reshape(lines, LANES),
            filter_bits.reshape(n, key_hi // n, key_lo),
            categories.reshape(own // LANES, LANES),
            attributes,
        )

    split = P(("fact", "dim"))
    return jax.shard_map(
        per_device,
        mesh=mesh,
        in_specs=(split, split, P(), split, P(("fact", "dim"), None)),
        out_specs=P(("fact", "dim"), None),
        check_vma=False,
    )
```

```python
import functools
import math

import jax
import jax.numpy as jnp
from jax import lax
from jax.experimental import pallas as pl
from jax.experimental.pallas import tpu as pltpu
from jax.sharding import PartitionSpec as P

CATS = 512
LANES = 128
MESH = pl.DeviceIdType.MESH


def rows_of(row, count):
    packed = jnp.broadcast_to(row, (16, LANES)).astype(jnp.bfloat16)
    return jnp.concatenate([packed] * (count // 16), axis=0)


def ids_of(count):
    return lax.broadcasted_iota(jnp.int32, (count, LANES), 0).astype(jnp.float32).astype(jnp.bfloat16)


def encode(sums, middle, rate):
    blocks = [sums[:, c : c + LANES] for c in range(0, sums.shape[1], LANES)]
    stacked = jnp.concatenate(blocks, axis=0)
    code = jnp.floor((jnp.log2(stacked) - middle) * rate + 0.5)
    return jnp.where(stacked > 0, code, -32768.0).astype(jnp.int32).astype(jnp.int16)


def decode(codes, middle, rate):
    wide = codes.astype(jnp.int32)
    return jnp.where(wide > -32768, jnp.exp2(wide.astype(jnp.float32) * (1 / rate) + middle), 0.0)


def kernel(
    n_fact,
    n_dim,
    keys_hbm,
    rev_hbm,
    filt_hbm,
    cat_hbm,
    attr_hbm,
    out_ref,
    keys_ref,
    rev_ref,
    high_ref,
    low_ref,
    value_ref,
    acc_ref,
    filt_ref,
    cat_ref,
    attr_ref,
    hot_ref,
    weight_ref,
    local1,
    pair1,
    whole1,
    send1,
    recv1,
    local2,
    pair2,
    send2,
    recv2,
    load_sem,
    pair_sem,
    send_sem1,
    recv_sem1,
    send_sem2,
    recv_sem2,
):
    n = n_fact * n_dim
    chips = n // 2
    me = lax.axis_index("fact") * n_dim + lax.axis_index("dim")
    core, chip = lax.rem(me, 2), me // 2
    partner = me + 1 - 2 * core
    key_hi, key_lo = acc_ref.shape
    own_rows = key_hi // n
    cat_rows = CATS // n

    def device(peer):
        return (peer // n_dim, lax.rem(peer, n_dim))

    bits = [1 << b for b in range(chips.bit_length() - 1)]
    flips = chips == 1 << len(bits)

    def chip_at(step):
        if not flips:
            return lax.rem(chip + step, chips)
        peer = 0
        for bit in bits:
            digit = lax.rem(chip // bit, 2)
            peer += (1 - digit if step & bit else digit) * bit
        return peer

    def source_at(step):
        return chip_at(step) if flips else lax.rem(chip + chips - step, chips)

    targets = [chip_at(step) for step in range(1, chips)][::-1]
    sources = [source_at(step) for step in range(1, chips)]

    first_loads = [
        pltpu.make_async_copy(keys_hbm, keys_ref, load_sem.at[3]),
        pltpu.make_async_copy(rev_hbm, rev_ref, load_sem.at[4]),
    ]
    for load in first_loads:
        load.start()
    loads = [
        pltpu.make_async_copy(attr_hbm, attr_ref, load_sem.at[0]),
        pltpu.make_async_copy(filt_hbm.at[me], filt_ref, load_sem.at[1]),
        pltpu.make_async_copy(cat_hbm, cat_ref, load_sem.at[2]),
    ]
    barrier = pltpu.get_barrier_semaphore()
    for peer in [partner] + [t * 2 + core for t in targets]:
        pl.semaphore_signal(barrier, inc=1, device_id=device(peer), device_id_type=MESH)

    for load in loads:
        load.start()
    for load in first_loads:
        load.wait()
    keys = keys_ref[...]
    high_ref[...] = (keys // key_lo).astype(jnp.float32)
    low_ref[...] = lax.rem(keys, key_lo).astype(jnp.float32)
    value_ref[...] = rev_ref[...].astype(jnp.float32)
    acc_ref[...] = jnp.zeros_like(acc_ref)

    lines = keys_ref.shape[0]
    step_lines = math.gcd(lines, 128)
    one = jnp.ones((), jnp.bfloat16)
    zero = jnp.zeros((), jnp.bfloat16)

    def add_block(block, carry):
        high_ids = ids_of(key_hi)
        low_ids = ids_of(key_lo)
        hots, weighted = [], []
        for j in range(step_lines):
            line = pl.ds(block * step_lines + j, 1)
            high = rows_of(high_ref[line, :], key_hi)
            low = rows_of(low_ref[line, :], key_lo)
            value = rows_of(value_ref[line, :], key_lo)
            hots.append(jnp.where(high == high_ids, one, zero))
            weighted.append(jnp.where(low == low_ids, value, zero))
        acc_ref[...] += lax.dot_general(
            jnp.concatenate(hots, axis=1),
            jnp.concatenate(weighted, axis=1),
            (((1,), (1,)), ((), ())),
            preferred_element_type=jnp.float32,
        )
        return carry

    lax.fori_loop(0, lines // step_lines, add_block, 0)

    for o in range(n):
        local1[o % 2, o // 2] = acc_ref[o * own_rows : (o + 1) * own_rows, :]

    pl.semaphore_wait(barrier, chips)

    least, most = -3.5, math.log2(2 * lines * LANES) + 0.5
    middle, rate = (least + most) / 2, 65000 / (most - least)

    def exchange(local, pair, send, recv, sems, send_sem, recv_sem, whole=None):
        swap = pltpu.make_async_remote_copy(
            src_ref=local.at[1 - core],
            dst_ref=pair,
            send_sem=pair_sem.at[sems],
            recv_sem=pair_sem.at[sems + 1],
            device_id=device(partner),
            device_id_type=MESH,
        )
        swap.start()
        swap.wait_recv()
        if whole is None:
            send[...] = local[core] + pair[...]
        else:
            whole[...] = local[core] + pair[...]
            for i in range(chips):
                send[i] = encode(whole[i], middle, rate)
        copies = [
            pltpu.make_async_remote_copy(
                src_ref=send.at[peer],
                dst_ref=recv.at[chip],
                send_sem=send_sem.at[peer],
                recv_sem=recv_sem.at[chip],
                device_id=device(peer * 2 + core),
                device_id_type=MESH,
            )
            for peer in targets
        ]
        for copy in copies:
            copy.start()

        def receive():
            if whole is None:
                total = send[chip]
            else:
                own = whole[chip]
                blocks = [own[:, c : c + LANES] for c in range(0, own.shape[1], LANES)]
                total = jnp.concatenate(blocks, axis=0)
            for peer in sources:
                pltpu.make_async_remote_copy(
                    src_ref=send.at[peer],
                    dst_ref=recv.at[peer],
                    send_sem=send_sem.at[peer],
                    recv_sem=recv_sem.at[peer],
                    device_id=device(peer * 2 + core),
                    device_id_type=MESH,
                ).wait_recv()
                total += recv[peer] if whole is None else decode(recv[peer], middle, rate)
            return total

        def finish():
            swap.wait_send()
            for copy in copies:
                copy.wait_send()

        return receive, finish

    receive1, finish1 = exchange(local1, pair1, send1, recv1, 0, send_sem1, recv_sem1, whole1)
    for load in loads:
        load.wait()

    half = CATS // 2
    ids = ids_of(half)
    per_row = key_lo // LANES
    chunks = own_rows * per_row
    for j in range(chunks):
        cat = cat_ref[j : j + 1, :]
        for h, local in enumerate((jnp.where(cat < half, cat, -1), cat - half)):
            hot_ref[h * half : (h + 1) * half, j * LANES : (j + 1) * LANES] = jnp.where(
                rows_of(local.astype(jnp.float32), half) == ids, one, zero
            )

    filt = [filt_ref[:, c * LANES : (c + 1) * LANES] for c in range(per_row)]
    sums = jnp.where(jnp.concatenate(filt, axis=0) == 1, receive1(), 0.0)
    stacked = [sums, jnp.zeros((LANES - chunks, LANES), jnp.float32)]
    columns = jnp.concatenate(stacked, axis=0).T
    width = attr_ref.shape[1]
    for j in range(chunks):
        i = j % per_row * own_rows + j // per_row
        keys_at = slice(j * LANES, (j + 1) * LANES)
        product = columns[:, i : i + 1] * attr_ref[keys_at, :].astype(jnp.float32)
        first = product.astype(jnp.bfloat16)
        weight_ref[keys_at, :width] = first
        weight_ref[keys_at, width:] = (product - first.astype(jnp.float32)).astype(jnp.bfloat16)
    both = jnp.dot(hot_ref[...], weight_ref[...], preferred_element_type=jnp.float32)
    totals = both[:, :width] + both[:, width:]
    for o in range(n):
        local2[o % 2, o // 2] = totals[o * cat_rows : (o + 1) * cat_rows, :]
    receive2, finish2 = exchange(local2, pair2, send2, recv2, 2, send_sem2, recv_sem2)
    finish1()
    out_ref[...] = receive2()
    finish2()


def solution(mesh):
    n_fact, n_dim = mesh.shape["fact"], mesh.shape["dim"]
    n = n_fact * n_dim

    def per_device(fact_keys, revenue, filter_bits, categories, attributes):
        rows = fact_keys.shape[0]
        key_hi, key_lo = filter_bits.shape
        own, width = attributes.shape
        lines = rows // LANES
        chips = n // 2
        sums_shape = (chips, key_hi // n, key_lo)
        part_shape = (chips, CATS // n, width)
        vmem = pl.BlockSpec(memory_space=pltpu.VMEM)
        hbm = pl.BlockSpec(memory_space=pl.ANY)
        codes = pltpu.VMEM((chips, own // LANES, LANES), jnp.int16)
        exchanged = [pltpu.VMEM((2,) + sums_shape, jnp.float32)]
        exchanged += [pltpu.VMEM(sums_shape, jnp.float32)] * 2 + [codes] * 2
        exchanged += [pltpu.VMEM((2,) + part_shape, jnp.float32)]
        exchanged += [pltpu.VMEM(part_shape, jnp.float32)] * 3
        return pl.pallas_call(
            functools.partial(kernel, n_fact, n_dim),
            out_shape=jax.ShapeDtypeStruct((CATS // n, width), jnp.float32),
            in_specs=[hbm] * 5,
            out_specs=vmem,
            scratch_shapes=[
                pltpu.VMEM((lines, LANES), jnp.int32),
                pltpu.VMEM((lines, LANES), jnp.bfloat16),
                pltpu.VMEM((lines, LANES), jnp.float32),
                pltpu.VMEM((lines, LANES), jnp.float32),
                pltpu.VMEM((lines, LANES), jnp.float32),
                pltpu.VMEM((key_hi, key_lo), jnp.float32),
                pltpu.VMEM((key_hi // n, key_lo), jnp.int32),
                pltpu.VMEM((own // LANES, LANES), jnp.int32),
                pltpu.VMEM((own, width), jnp.bfloat16),
                pltpu.VMEM((CATS, own), jnp.bfloat16),
                pltpu.VMEM((own, 2 * width), jnp.bfloat16),
            ]
            + exchanged
            + [pltpu.SemaphoreType.DMA((5,)), pltpu.SemaphoreType.DMA((4,))]
            + [pltpu.SemaphoreType.DMA((chips,))] * 4,
            compiler_params=pltpu.CompilerParams(collective_id=0, has_side_effects=True),
        )(
            fact_keys.reshape(lines, LANES),
            revenue.reshape(lines, LANES),
            filter_bits.reshape(n, key_hi // n, key_lo),
            categories.reshape(own // LANES, LANES),
            attributes,
        )

    split = P(("fact", "dim"))
    return jax.shard_map(
        per_device,
        mesh=mesh,
        in_specs=(split, split, P(), split, P(("fact", "dim"), None)),
        out_specs=P(("fact", "dim"), None),
        check_vma=False,
    )
```
